32 devices in a mesh: dp: 4 (over y, x), centers: 8 (over z, core).
Axes of the slice: x: 2, y: 2, z: 4, core: 2. Of those that a mesh axis runs over, the one named last changes fastest.
Arguments:
- points: bfloat16 [16384, 32], P('dp'), may hold values from -6 to 6
- centers: bfloat16 [16384, 32], P('centers'), may hold values from -6 to 6
- coef: bfloat16 [16384, 64], P('centers'), may hold values from -0.1875 to 0.1875
Outputs:
- product: float32 [16384, 64], P('centers')
The draws below stay inside these ranges and needn't reach their ends.
All inputs are finite; a program needn't handle non-finite values.
Results may differ from the reference program's by a relative error of at most 0.0003.
Values may be sent and summed in bfloat16 or wider, within the bound.
A program may use at most 128 MiB of HBM per device.

```python
import jax
import jax.numpy as jnp
from jax import lax

DIM = 32
OUTS = 64
NPTS = 16384
CENTERS = 16384


def block_scale(key, shape, shards, low, top_value):
    gain, own = 1.0, jax.random.fold_in(key, 6)
    for axis_at, blocks in shards:
        heights = jnp.exp(jax.random.uniform(jax.random.fold_in(own, axis_at), (blocks,), jnp.float32, low / len(shards), top_value / len(shards)))
        gain = gain * jnp.repeat(heights, shape[axis_at] // blocks).reshape([-1 if axis == axis_at else 1 for axis in range(len(shape))])
    return gain


def scatter_about(rng, shape, scale, limit, cuts=(), kind=jnp.bfloat16):
    values = jax.random.normal(rng, shape, jnp.float32) * scale
    if len(cuts) > 0:
        values = block_scale(rng, shape, cuts, -0.22, 0.18) * values
    return jnp.clip(values, min=-limit, max=limit).astype(kind)


def setup_inputs(seed: int = 0) -> dict:
    key_list = jax.random.split(jax.random.key(seed), 4)
    return {
        "points": scatter_about(key_list[0], (NPTS, DIM), 1.0, 6.0, ((0, 4),)),
        "centers": scatter_about(key_list[1], (CENTERS, DIM), 1.0, 6.0, ((0, 8),)),
        "coef": scatter_about(key_list[2], (CENTERS, OUTS), (CENTERS // 16) ** -0.5, 0.1875, ((0, 8),)),
    }


def kernel_block(left_pts, left_sq, right_pts, right_sq, features):
    inner = lax.dot_general(left_pts, right_pts, (((1,), (1,)), ((), ())), preferred_element_type=jnp.float32)
    dist = left_sq[:, None] + right_sq[None, :] - 2.0 * inner
    return jnp.exp(dist * (-2.0 / features)).astype(jnp.bfloat16)

def squares(values):
    wide = values.astype(jnp.float32)
    return lax.optimization_barrier(jnp.sum(wide * wide, axis=1))

def reference(points, centers, coef):
    features = points.shape[1]
    total_pts = points.shape[0]
    total_cen = centers.shape[0]
    outs_count = coef.shape[1]
    block_pts = min(1024, total_pts)
    cen_sq = squares(centers)
    point_blocks = points.reshape(total_pts // block_pts, block_pts, features)

    def data_step(accum, block):
        kernel = kernel_block(block, squares(block), centers, cen_sq, features)
        forward = jnp.dot(kernel, coef, preferred_element_type=jnp.float32).astype(jnp.bfloat16)
        back = lax.dot_general(kernel, forward, (((0,), (0,)), ((), ())), preferred_element_type=jnp.float32)
        return (accum + back, jnp.zeros((), jnp.float32))
    accum, unused = lax.scan(data_step, jnp.zeros((total_cen, outs_count), jnp.float32), point_blocks)
    block_cen = min(1024, total_cen)
    center_blocks = centers.reshape(total_cen // block_cen, block_cen, features)

    def center_step(carry, block):
        kernel = kernel_block(block, squares(block), centers, cen_sq, features)
        return (carry, jnp.dot(kernel, coef, preferred_element_type=jnp.float32))
    unused_two, regular = lax.scan(center_step, jnp.zeros((), jnp.float32), center_blocks)
    regular = regular.reshape(total_cen, outs_count)
    return accum * (1.0 / jnp.sqrt(jnp.float32(total_pts))) + regular
```

```python
import functools
import math

import jax
import jax.numpy as jnp
from jax import lax
from jax.experimental import pallas as pl
from jax.experimental.pallas import tpu as pltpu
from jax.sharding import PartitionSpec as P

MESH = pl.DeviceIdType.MESH
F32, BF16 = jnp.float32, jnp.bfloat16


def dot(a, b):
    return lax.dot_general(a, b, (((1,), (0,)), ((), ())), preferred_element_type=F32)


def dot_nt(a, b):
    return lax.dot_general(a, b, (((1,), (1,)), ((), ())), preferred_element_type=F32)


def split3(v):
    hi = v.astype(BF16).astype(F32)
    mid = (v - hi).astype(BF16).astype(F32)
    return hi, mid, (v - hi) - mid


def row_form(xt, width):
    feats, count = xt.shape
    wide = xt.astype(F32)
    sq = jnp.sum(wide * wide, axis=0, keepdims=True) * (-2.0 * math.log2(math.e) / feats)
    hi, mid, lo = split3(sq)
    at = lax.broadcasted_iota(jnp.int32, (width - 3 * feats, count), 0)
    tail = jnp.where(at == 3, hi, jnp.where(at == 4, mid, jnp.where(at == 5, lo, 0.0)))
    tail = jnp.where(at < 3, 1.0, tail)
    return jnp.concatenate([xt, xt, xt, tail.astype(BF16)], axis=0).T


def col_form(ct, width):
    feats, count = ct.shape
    wide = ct.astype(F32)
    parts = [p.astype(BF16) for p in split3(wide * (4.0 * math.log2(math.e) / feats))]
    sq = jnp.sum(wide * wide, axis=0, keepdims=True) * (-2.0 * math.log2(math.e) / feats)
    hi, mid, lo = split3(sq)
    at = lax.broadcasted_iota(jnp.int32, (width - 3 * feats, count), 0)
    tail = jnp.where(at == 0, hi, jnp.where(at == 1, mid, jnp.where(at == 2, lo, 0.0)))
    tail = jnp.where((at >= 3) & (at < 6), 1.0, tail)
    return jnp.concatenate(parts + [tail.astype(BF16)], axis=0)


def kern(rows, cols):
    return jnp.exp2(dot(rows, cols)).astype(BF16)


def body(cfg, pts_hbm, cen_hbm, coef_hbm, out, pts, packed, lsem, sibp, kmat, colt, rowc, gath, reg, own_half, snd1, rcv1, snd2, rcv2,
         own_sum, fwd, csend, crecv, cown, full,
         as_, ar, fs, fr, b1s, b1r, b2s, b2r, gs, gr, hs, hr, cs, cr, ds_, dr):
    n_dp, n_c, feats, width = cfg
    n_h = n_c // 2
    d = lax.axis_index("dp")
    j = lax.axis_index("centers")
    par = lax.rem(j, 2)
    z = j // 2
    sib = j + 1 - 2 * par
    local_pts = pts.shape[1]
    local_cen = packed.shape[1]
    share = local_pts // n_c
    quarter = local_cen // n_dp
    step = min(1024, local_cen)
    alpha_scale = 1.0 / math.sqrt(local_pts * n_dp)

    def up(t):
        return lax.rem(z + 1 + t, n_h)

    def down(t):
        return lax.rem(z + 2 * n_h - 1 - t, n_h)

    def dup(t):
        return lax.rem(d + 1 + t, n_dp)

    def ddown(t):
        return lax.rem(d + 2 * n_dp - 1 - t, n_dp)

    def copy(src, dst, ssem, rsem, dev):
        return pltpu.make_async_remote_copy(
            src_ref=src, dst_ref=dst, send_sem=ssem, recv_sem=rsem, device_id=dev, device_id_type=MESH
        )

    barrier = pltpu.get_barrier_semaphore()
    for t in range(n_h - 1):
        pl.semaphore_signal(barrier, inc=1, device_id=(d, 2 * up(t) + par), device_id_type=MESH)
    pl.semaphore_signal(barrier, inc=1, device_id=(d, sib), device_id_type=MESH)
    for t in range(n_dp - 1):
        pl.semaphore_signal(barrier, inc=1, device_id=(dup(t), j), device_id_type=MESH)

    cen_in = pltpu.make_async_copy(cen_hbm, packed.at[:feats], lsem.at[0])
    coef_in = pltpu.make_async_copy(coef_hbm, packed.at[feats:], lsem.at[1])
    pts_in = pltpu.make_async_copy(pts_hbm, pts, lsem.at[2])
    cen_in.start()
    coef_in.start()
    pts_in.start()
    cen_in.wait()
    for c in range(local_cen // step):
        at = pl.ds(c * step, step)
        colt[:, at] = col_form(packed[:feats, at], width)
    for c in range(local_cen // step):
        at = pl.ds(c * step, step)
        rowc[at, :] = row_form(packed[:feats, at], width)
    reg[...] = jnp.zeros_like(reg)

    pl.semaphore_wait(barrier, n_h - 1 + 1 + n_dp - 1)
    coef_in.wait()

    mine = packed.at[:, pl.ds(pl.multiple_of(d * quarter, 128), quarter)]

    def gather(t):
        return copy(mine, gath.at[j], as_.at[t], ar.at[t], (d, 2 * up(t) + par))

    def gather_in(t):
        return copy(mine, gath.at[2 * down(t) + par], as_.at[t], ar.at[t], (d, 2 * up(t) + par))

    for t in range(n_h - 1):
        gather(t).start()
    own_to_sib = copy(packed, sibp, fs.at[n_h - 1], fr.at[n_h - 1], (d, sib))
    own_to_sib.start()
    pts_in.wait()

    def to_sib(t):
        return copy(snd1.at[t], rcv1.at[t], b1s.at[t], b1r.at[t], (d, sib))

    def to_peer(t):
        return copy(snd2.at[t], rcv2.at[t], b2s.at[t], b2r.at[t], (d, 2 * up(t) + par))

    def half(s):
        at = pl.ds(pl.multiple_of(s * share, share), share)
        rows = row_form(pts[:, at], width)
        acc = jnp.zeros((packed.shape[0] - feats, share), F32)
        for c in range(local_cen // step):
            cols = pl.ds(c * step, step)
            tile = kern(rows, colt[:, cols])
            kmat[at, cols] = tile
            acc = acc + dot_nt(packed[feats:, cols], tile)
        return acc

    @pl.loop(0, n_h)
    def _(t):
        zt = up(t)
        snd1[t] = half(2 * zt + 1 - par).astype(BF16)
        to_sib(t).start()
        own_half[...] = half(2 * zt + par)
        to_sib(t).wait_recv()
        total = own_half[...] + rcv1[t].astype(F32)

        @pl.when(t < n_h - 1)
        def _():
            snd2[t] = total.astype(BF16)
            to_peer(t).start()

        @pl.when(t == n_h - 1)
        def _():
            own_sum[...] = total

    def forward_block(t):
        at = gath.at[2 * down(t) + par]
        return copy(at, at, fs.at[t], fr.at[t], (d, sib))

    def forward_in(t):
        at = gath.at[2 * down(t) + 1 - par]
        return copy(at, at, fs.at[t], fr.at[t], (d, sib))

    for t in range(n_h - 1):
        gather_in(t).wait_recv()
        forward_block(t).start()

    def regular(block):
        cols = col_form(gath[block, :feats, :], width)
        weights = gath[block, feats:, :]
        for r in range(local_cen // step):
            rows = pl.ds(r * step, step)
            reg[:, rows] += dot_nt(weights, kern(rowc[rows, :], cols))

    for t in range(n_h - 1):
        to_peer(t).wait_recv()
    total = own_sum[...]
    for t in range(n_h - 1):
        total = total + rcv2[t].astype(F32)

    def slot(s):
        return fwd.at[:, pl.ds(pl.multiple_of(s * share, share), share)]

    def spread(t):
        return copy(slot(j), slot(j), gs.at[t], gr.at[t], (d, 2 * up(t) + par))

    def spread_in(t):
        at = slot(2 * down(t) + par)
        return copy(at, at, gs.at[t], gr.at[t], (d, 2 * up(t) + par))

    fwd[:, pl.ds(pl.multiple_of(j * share, share), share)] = total.astype(BF16)
    for t in range(n_h - 1):
        spread(t).start()
    own_fwd = copy(slot(j), slot(j), hs.at[n_h - 1], hr.at[n_h - 1], (d, sib))
    own_fwd.start()

    @pl.loop(0, n_h - 1)
    def _(i):
        regular(2 * up(i) + par)

    for t in range(n_h - 1):
        forward_in(t).wait_recv()

    cut = ((n_h - 1) * 2) // 3

    @pl.loop(0, cut)
    def _(i):
        regular(2 * up(i) + 1 - par)

    def relay(t):
        at = slot(2 * down(t) + par)
        return copy(at, at, hs.at[t], hr.at[t], (d, sib))

    def relay_in(t):
        at = slot(2 * down(t) + 1 - par)
        return copy(at, at, hs.at[t], hr.at[t], (d, sib))

    for t in range(n_h - 1):
        spread_in(t).wait_recv()
        relay(t).start()

    @pl.loop(cut, n_h - 1)
    def _(i):
        regular(2 * up(i) + 1 - par)

    for t in range(n_h - 1):
        relay_in(t).wait_recv()
    copy(slot(sib), slot(sib), hs.at[n_h - 1], hr.at[n_h - 1], (d, sib)).wait_recv()

    def cross(t):
        return copy(csend.at[t], crecv.at[t], cs.at[t], cr.at[t], (dup(t), j))

    @pl.loop(0, n_dp)
    def _(t):
        at = pl.ds(pl.multiple_of(dup(t) * quarter, 128), quarter)
        back = dot(fwd[...], kmat[:, at]) * alpha_scale + reg[:, at]

        @pl.when(t < n_dp - 1)
        def _():
            csend[t] = back
            cross(t).start()

        @pl.when(t == n_dp - 1)
        def _():
            cown[...] = back

    own_to_sib.wait_recv()
    mine_rows = rowc[pl.ds(pl.multiple_of(d * quarter, 128), quarter), :]
    for c in range(local_cen // step):
        at = pl.ds(c * step, step)
        cown[...] += dot_nt(packed[feats:, at], kern(mine_rows, colt[:, at]))
        cown[...] += dot_nt(sibp[feats:, at], kern(mine_rows, col_form(sibp[:feats, at], width)))

    for t in range(n_dp - 1):
        cross(t).wait_recv()
    total = cown[...]
    for t in range(n_dp - 1):
        total = total + crecv[t]
    full[d] = total

    def publish(t):
        return copy(full.at[d], full.at[d], ds_.at[t], dr.at[t], (dup(t), j))

    def publish_in(t):
        at = full.at[ddown(t)]
        return copy(at, at, ds_.at[t], dr.at[t], (dup(t), j))

    for t in range(n_dp - 1):
        publish(t).start()
    for t in range(n_h - 1):
        gather(t).wait_send()
        forward_block(t).wait_send()
        to_peer(t).wait_send()
        spread(t).wait_send()
        relay(t).wait_send()
    for t in range(n_h):
        to_sib(t).wait_send()
    own_to_sib.wait_send()
    own_fwd.wait_send()
    for t in range(n_dp - 1):
        cross(t).wait_send()
    for t in range(n_dp - 1):
        publish_in(t).wait_recv()
    for t in range(n_dp - 1):
        publish(t).wait_send()
    for q in range(n_dp):
        out[:, q * quarter:(q + 1) * quarter] = full[q]


def solution(mesh):
    n_dp, n_c = mesh.shape["dp"], mesh.shape["centers"]

    def on_device(points, centers, coef):
        local_pts, feats = points.shape
        local_cen, outs = coef.shape
        width = -(-(3 * feats + 6) // 128) * 128
        n_h = n_c // 2
        share, quarter = local_pts // n_c, local_cen // n_dp
        dma = pltpu.SemaphoreType.DMA
        result = pl.pallas_call(
            functools.partial(body, (n_dp, n_c, feats, width)),
            out_shape=jax.ShapeDtypeStruct((outs, local_cen), F32),
            in_specs=[pl.BlockSpec(memory_space=pl.ANY)] * 3,
            out_specs=pl.BlockSpec(memory_space=pltpu.VMEM),
            scratch_shapes=[
                pltpu.VMEM((feats, local_pts), BF16),
                pltpu.VMEM((feats + outs, local_cen), BF16),
                dma((3,)),
                pltpu.VMEM((feats + outs, local_cen), BF16),
                pltpu.VMEM((local_pts, local_cen), BF16),
                pltpu.VMEM((width, local_cen), BF16),
                pltpu.VMEM((local_cen, width), BF16),
                pltpu.VMEM((n_c, feats + outs, quarter), BF16),
                pltpu.VMEM((outs, local_cen), F32),
                pltpu.VMEM((outs, share), F32),
                pltpu.VMEM((n_h, outs, share), BF16),
                pltpu.VMEM((n_h, outs, share), BF16),
                pltpu.VMEM((n_h, outs, share), BF16),
                pltpu.VMEM((n_h, outs, share), BF16),
                pltpu.VMEM((outs, share), F32),
                pltpu.VMEM((outs, local_pts), BF16),
                pltpu.VMEM((n_dp, outs, quarter), F32),
                pltpu.VMEM((n_dp, outs, quarter), F32),
                pltpu.VMEM((outs, quarter), F32),
                pltpu.VMEM((n_dp, outs, quarter), F32),
            ] + [dma((n_h,))] * 12 + [dma((n_dp,))] * 4,
            compiler_params=pltpu.CompilerParams(
                collective_id=0, has_side_effects=True, vmem_limit_bytes=60 * 1024 * 1024
            ),
        )(points.T, centers.T, coef.T)
        return result.T

    return jax.shard_map(
        on_device,
        mesh=mesh,
        in_specs=(P("dp", None), P("centers", None), P("centers", None)),
        out_specs=P("centers", None),
        check_vma=False,
    )
```

```python
import functools
import math

import jax
import jax.numpy as jnp
from jax import lax
from jax.experimental import pallas as pl
from jax.experimental.pallas import tpu as pltpu
from jax.sharding import PartitionSpec as P

MESH = pl.DeviceIdType.MESH
F32, BF16 = jnp.float32, jnp.bfloat16
PIECE = 512


def dot(a, b):
    return lax.dot_general(a, b, (((1,), (0,)), ((), ())), preferred_element_type=F32)


def dot_nt(a, b):
    return lax.dot_general(a, b, (((1,), (1,)), ((), ())), preferred_element_type=F32)


def split3(v):
    hi = v.astype(BF16).astype(F32)
    mid = (v - hi).astype(BF16).astype(F32)
    return hi, mid, (v - hi) - mid


def row_form(xt, width):
    feats, count = xt.shape
    wide = xt.astype(F32)
    sq = jnp.sum(wide * wide, axis=0, keepdims=True) * (-2.0 * math.log2(math.e) / feats)
    hi, mid, lo = split3(sq)
    at = lax.broadcasted_iota(jnp.int32, (width - 3 * feats, count), 0)
    tail = jnp.where(at == 3, hi, jnp.where(at == 4, mid, jnp.where(at == 5, lo, 0.0)))
    tail = jnp.where(at < 3, 1.0, tail)
    return jnp.concatenate([xt, xt, xt, tail.astype(BF16)], axis=0).T


def col_form(ct, width):
    feats, count = ct.shape
    wide = ct.astype(F32)
    parts = [p.astype(BF16) for p in split3(wide * (4.0 * math.log2(math.e) / feats))]
    sq = jnp.sum(wide * wide, axis=0, keepdims=True) * (-2.0 * math.log2(math.e) / feats)
    hi, mid, lo = split3(sq)
    at = lax.broadcasted_iota(jnp.int32, (width - 3 * feats, count), 0)
    tail = jnp.where(at == 0, hi, jnp.where(at == 1, mid, jnp.where(at == 2, lo, 0.0)))
    tail = jnp.where((at >= 3) & (at < 6), 1.0, tail)
    return jnp.concatenate(parts + [tail.astype(BF16)], axis=0)


def xor(v, k):
    out, bit = v, 1
    while bit <= k:
        if k & bit:
            out = out + bit - 2 * bit * lax.rem(v // bit, 2)
        bit *= 2
    return out


def staggered(pieces, lag=1):
    held = []
    for logits, apply in pieces:
        e = logits()
        if len(held) == lag:
            tile, use = held.pop(0)
            use(tile)
        held.append((jnp.exp2(e).astype(BF16), apply))
    for tile, use in held:
        use(tile)


def body(cfg, pts_hbm, cen_hbm, coef_hbm, out, pts, packed, lsem, sibp, kmat, colt, gath, reg, own_half, snd1, rcv1, snd2, rcv2,
         own_sum, fwd, csend, crecv, cown, full, rowp, loc,
         os_, or_, b1s, b1r, b2s, b2r, gs, gr, hs, hr, ups, upr, dns, dnr, fus, fur, fds, fdr, cs, cr, ds_, dr):
    n_dp, n_c, feats, width, n_ck, n_cc = cfg
    n_h = n_c // 2
    d = lax.axis_index("dp")
    j = lax.axis_index("centers")
    par = lax.rem(j, 2)
    z = j // 2
    sib = j + 1 - 2 * par
    local_pts = pts.shape[1]
    local_cen = packed.shape[1]
    outs = packed.shape[0] - feats
    share = local_pts // n_c
    sh = share // n_ck
    span = n_c * sh
    quarter = local_cen // n_dp
    cw = quarter // n_cc
    piece = min(PIECE, local_cen)
    alpha_scale = 1.0 / math.sqrt(local_pts * n_dp)

    def copy(src, dst, ssem, rsem, dev):
        return pltpu.make_async_remote_copy(
            src_ref=src, dst_ref=dst, send_sem=ssem, recv_sem=rsem, device_id=dev, device_id_type=MESH
        )

    def peer(k):
        return (d, 2 * xor(z, k) + par)

    barrier = pltpu.get_barrier_semaphore()
    for k in range(1, n_h):
        pl.semaphore_signal(barrier, inc=1, device_id=peer(k), device_id_type=MESH)
    pl.semaphore_signal(barrier, inc=1, device_id=(d, sib), device_id_type=MESH)
    for k in range(1, n_dp):
        pl.semaphore_signal(barrier, inc=1, device_id=(xor(d, k), j), device_id_type=MESH)

    cen_in = pltpu.make_async_copy(cen_hbm, packed.at[:feats], lsem.at[0])
    coef_in = pltpu.make_async_copy(coef_hbm, packed.at[feats:], lsem.at[1])
    pts_in = pltpu.make_async_copy(pts_hbm, pts, lsem.at[2])
    cen_in.start()
    coef_in.start()
    pts_in.start()
    cen_in.wait()
    for c in range(local_cen // piece):
        at = pl.ds(c * piece, piece)
        colt[:, at] = col_form(packed[:feats, at], width)
    reg[...] = jnp.zeros_like(reg)
    loc[...] = jnp.zeros_like(loc)
    coef_in.wait()
    pts_in.wait()

    mine = packed.at[:, pl.ds(pl.multiple_of(d * quarter, 128), quarter)]

    def up(r):
        dst = gath.at[2 * (z - r) + par]
        return copy(mine if r == 0 else dst, dst, ups.at[r], upr.at[r], (d, 2 * (z + 1) + par))

    def down(r):
        dst = gath.at[2 * (z + r) + par]
        return copy(mine if r == 0 else dst, dst, dns.at[r], dnr.at[r], (d, 2 * (z - 1) + par))

    def up_in(r):
        dst = gath.at[2 * (z - r) + par]
        return copy(dst, dst, ups.at[r - 1], upr.at[r - 1], (d, sib))

    def down_in(r):
        dst = gath.at[2 * (z + r) + par]
        return copy(dst, dst, dns.at[r - 1], dnr.at[r - 1], (d, sib))

    def below_sib(r):
        at = gath.at[2 * (z - r) + par]
        return copy(at, at, fus.at[r], fur.at[r], (d, sib))

    def above_sib(r):
        at = gath.at[2 * (z + r) + par]
        return copy(at, at, fds.at[r], fdr.at[r], (d, sib))

    def below_sib_in(r):
        at = gath.at[2 * (z - r) + 1 - par]
        return copy(at, at, fus.at[r], fur.at[r], (d, sib))

    def above_sib_in(r):
        at = gath.at[2 * (z + r) + 1 - par]
        return copy(at, at, fds.at[r], fdr.at[r], (d, sib))

    def hop(r):
        if r > 0:
            @pl.when(z >= r)
            def _():
                up_in(r).wait_recv()
                below_sib(r).start()

            @pl.when(z + r < n_h)
            def _():
                down_in(r).wait_recv()
                above_sib(r).start()

        if r < n_h - 1:
            @pl.when((z >= r) & (z < n_h - 1))
            def _():
                up(r).start()

            @pl.when((z + r < n_h) & (z > 0))
            def _():
                down(r).start()

    def hop_sib_in(r):
        @pl.when(z >= r)
        def _():
            below_sib_in(r).wait_recv()

        @pl.when(z + r < n_h)
        def _():
            above_sib_in(r).wait_recv()

    def hop_sent(r):
        if r > 0:
            @pl.when(z >= r)
            def _():
                below_sib(r).wait_send()

            @pl.when(z + r < n_h)
            def _():
                above_sib(r).wait_send()

        if r < n_h - 1:
            @pl.when((z >= r) & (z < n_h - 1))
            def _():
                up(r).wait_send()

            @pl.when((z + r < n_h) & (z > 0))
            def _():
                down(r).wait_send()

    own_to_sib = copy(packed, sibp, os_.at[0], or_.at[0], (d, sib))

    def to_sib(s):
        return copy(snd1.at[s], rcv1.at[s], b1s.at[s], b1r.at[s], (d, sib))

    def to_peer(c, k):
        i = c * n_h + k
        return copy(snd2.at[i], rcv2.at[i], b2s.at[i], b2r.at[i], peer(k))

    def slot(c, q):
        return fwd.at[:, pl.ds(pl.multiple_of(c * span + q * sh, sh), sh)]

    def spread(c, k):
        i = c * n_h + k
        return copy(slot(c, j), slot(c, j), gs.at[i], gr.at[i], peer(k))

    def spread_in(c, k):
        i = c * n_h + k
        at = slot(c, 2 * xor(z, k) + par)
        return copy(at, at, gs.at[i], gr.at[i], peer(k))

    def relay(c, k):
        i = c * n_h + k
        at = slot(c, 2 * xor(z, k) + par)
        return copy(at, at, hs.at[i], hr.at[i], (d, sib))

    def relay_in(c, k):
        i = c * n_h + k
        at = slot(c, 2 * xor(z, k) + 1 - par)
        return copy(at, at, hs.at[i], hr.at[i], (d, sib))

    steps = n_ck * n_h

    group = 2

    def owners(s):
        zt = xor(z, n_h - 1 - s % n_h)
        return 2 * zt + 1 - par, 2 * zt + par

    def point_rows(g):
        for i, s in enumerate(range(g * group, (g + 1) * group)):
            for h, q in enumerate(owners(s)):
                src = pl.ds(pl.multiple_of(q * share + (s // n_h) * sh, sh), sh)
                rowp[g % 2, i, h * sh:(h + 1) * sh, :] = row_form(pts[:, src], width)

    def forward(g):
        if (g + 1) * group < steps:
            point_rows(g + 1)
        pieces = []
        accs = []
        for i, s in enumerate(range(g * group, (g + 1) * group)):
            acc = [jnp.zeros((outs, 2 * sh), F32)]
            accs.append(acc)
            ats = [pl.ds(pl.multiple_of((s // n_h) * span + q * sh, sh), sh) for q in owners(s)]
            for b in range(local_cen // piece):
                cols = pl.ds(b * piece, piece)

                def logits(i=i, cols=cols):
                    return dot(rowp[g % 2, i], colt[:, cols])

                def apply(tile, acc=acc, ats=ats, cols=cols):
                    for h in range(2):
                        kmat[ats[h], cols] = tile[h * sh:(h + 1) * sh]
                    acc[0] = acc[0] + dot_nt(packed[feats:, cols], tile)

                pieces.append((logits, apply))
        staggered(pieces)
        for acc, s in zip(accs, range(g * group, (g + 1) * group)):
            snd1[s] = acc[0][:, :sh].astype(BF16)
            own_half[s] = acc[0][:, sh:]

    def combine(s):
        c, k = s // n_h, n_h - 1 - s % n_h
        to_sib(s).wait_recv()
        total = own_half[s] + rcv1[s].astype(F32)
        if k > 0:
            snd2[c * n_h + k] = total.astype(BF16)
            to_peer(c, k).start()
        else:
            own_sum[c] = total

    def finish(c):
        for k in range(1, n_h):
            to_peer(c, k).wait_recv()
        total = own_sum[c]
        for k in range(1, n_h):
            total = total + rcv2[c * n_h + k].astype(F32)
        slot(c, j)[...] = total.astype(BF16)
        for k in reversed(range(1, n_h)):
            spread(c, k).start()
        relay(c, 0).start()

    def relays(c):
        for k in range(1, n_h):
            spread_in(c, k).wait_recv()
            relay(c, k).start()

    def regular(*blocks):
        pieces = []
        for block in blocks:
            rows = row_form(gath[block, :feats, :], width)
            weights = gath[block, feats:, :]
            for r in range(0, quarter, 256):
                part = slice(r, r + 256)
                for b in range(local_cen // piece):
                    cols = pl.ds(b * piece, piece)

                    def logits(rows=rows[part], cols=cols):
                        return dot(rows, colt[:, cols])

                    def apply(tile, weights=weights[:, part], cols=cols):
                        reg[:, cols] += dot(weights, tile)

                    pieces.append((logits, apply))
        staggered(pieces, 2)

    def back(c, at):
        rows = pl.ds(c * span, span)
        return dot(fwd[:, rows], kmat[rows, at]) * alpha_scale

    hops = list(range(1, n_h))
    sib_hops = list(range(1, n_h))

    def ensure(r):
        while hops and hops[0] <= r:
            hop(hops.pop(0))

    def ensure_sib(r):
        ensure(r)
        while sib_hops and sib_hops[0] <= r:
            hop_sib_in(sib_hops.pop(0))

    own_cols = pl.ds(pl.multiple_of(d * quarter, 128), quarter)

    def local(src):
        total = [loc[...]]
        pieces = []
        for b in range(local_cen // piece):
            at = pl.ds(b * piece, piece)

            def logits(at=at):
                return dot(row_form(src[:feats, at], width), colt[:, own_cols])

            def apply(tile, at=at):
                total[0] = total[0] + dot(src[feats:, at], tile)

            pieces.append((logits, apply))
        staggered(pieces)
        loc[...] = total[0]

    last = n_ck - 1
    groups = steps // group
    point_rows(0)
    for g in range(groups):
        forward(g)
        if g == 0:
            pl.semaphore_wait(barrier, n_h - 1 + 1 + n_dp - 1)
        for s in range(g * group, (g + 1) * group):
            to_sib(s).start()
        if g == 0:
            hop(0)
        if g > 0:
            for s in range((g - 1) * group, g * group):
                combine(s)
        if g == groups - 2:
            ensure(1)
            own_to_sib.start()
    near = 2 * xor(z, 1)
    ensure_sib(1)
    regular(near + par)
    for s in range(steps - group, steps):
        combine(s)
    if n_ck > 1:
        finish(0)
    regular(near + 1 - par)
    local(packed)
    ensure(2)
    finish(last)
    own_to_sib.wait_recv()
    local(sibp)
    rest = list(range(2, n_h))
    for k in rest[:-1]:
        ensure(k)
        regular(2 * xor(z, k) + par)
        ensure_sib(k)
        regular(2 * xor(z, k) + 1 - par)
    if n_ck > 1:
        relays(0)
        for k in range(n_h):
            relay_in(0, k).wait_recv()
        for b in range(local_cen // piece):
            cols = pl.ds(b * piece, piece)
            reg[:, cols] += back(0, cols)
    for k in rest[-1:]:
        ensure(k)
        relays(last)
        ensure_sib(k)
        regular(2 * xor(z, k) + par, 2 * xor(z, k) + 1 - par)
    if not rest:
        relays(last)
    for k in range(n_h):
        relay_in(last, k).wait_recv()

    def cross(cc, k):
        i = cc * n_dp + k
        return copy(csend.at[i], crecv.at[i], cs.at[i], cr.at[i], (xor(d, k), j))

    for cc in range(n_cc):
        for k in reversed(range(n_dp)):
            at = pl.ds(pl.multiple_of(xor(d, k) * quarter + cc * cw, 128), cw)
            total = back(last, at) + reg[:, at]
            if k > 0:
                csend[cc * n_dp + k] = total
            else:
                cown[cc] = total + loc[:, cc * cw:(cc + 1) * cw]
        for k in reversed(range(1, n_dp)):
            cross(cc, k).start()

    def publish(cc, k):
        i = cc * n_dp + k
        at = full.at[cc, d]
        return copy(at, at, ds_.at[i], dr.at[i], (xor(d, k), j))

    def publish_in(cc, k):
        i = cc * n_dp + k
        at = full.at[cc, xor(d, k)]
        return copy(at, at, ds_.at[i], dr.at[i], (xor(d, k), j))

    for cc in range(n_cc):
        for k in range(1, n_dp):
            cross(cc, k).wait_recv()
        total = cown[cc]
        for k in range(1, n_dp):
            total = total + crecv[cc * n_dp + k]
        full[cc, d] = total
        for k in reversed(range(1, n_dp)):
            publish(cc, k).start()

    for r in range(n_h):
        hop_sent(r)
    for s in range(steps):
        to_sib(s).wait_send()
    own_to_sib.wait_send()
    for c in range(n_ck):
        relay(c, 0).wait_send()
        for k in range(1, n_h):
            to_peer(c, k).wait_send()
            spread(c, k).wait_send()
            relay(c, k).wait_send()
    for cc in range(n_cc):
        for k in range(1, n_dp):
            cross(cc, k).wait_send()
            publish_in(cc, k).wait_recv()
        for q in range(n_dp):
            out[:, q * quarter + cc * cw:q * quarter + (cc + 1) * cw] = full[cc, q]
    for cc in range(n_cc):
        for k in range(1, n_dp):
            publish(cc, k).wait_send()


def solution(mesh):
    n_dp, n_c = mesh.shape["dp"], mesh.shape["centers"]

    def on_device(points, centers, coef):
        local_pts, feats = points.shape
        local_cen, outs = coef.shape
        width = -(-(3 * feats + 6) // 128) * 128
        n_h = n_c // 2
        share, quarter = local_pts // n_c, local_cen // n_dp
        n_ck = 2 if share % 256 == 0 else 1
        n_cc = 2 if quarter % 256 == 0 else 1
        sh, cw = share // n_ck, quarter // n_cc
        dma = pltpu.SemaphoreType.DMA
        args = [pltpu.with_memory_space_constraint(v.T, pltpu.HBM) for v in (points, centers, coef)]
        result = pl.pallas_call(
            functools.partial(body, (n_dp, n_c, feats, width, n_ck, n_cc)),
            out_shape=jax.ShapeDtypeStruct((outs, local_cen), F32),
            in_specs=[pl.BlockSpec(memory_space=pl.ANY)] * 3,
            out_specs=pl.BlockSpec(memory_space=pltpu.VMEM),
            scratch_shapes=[
                pltpu.VMEM((feats, local_pts), BF16),
                pltpu.VMEM((feats + outs, local_cen), BF16),
                dma((3,)),
                pltpu.VMEM((feats + outs, local_cen), BF16),
                pltpu.VMEM((local_pts, local_cen), BF16),
                pltpu.VMEM((width, local_cen), BF16),
                pltpu.VMEM((n_c, feats + outs, quarter), BF16),
                pltpu.VMEM((outs, local_cen), F32),
                pltpu.VMEM((n_ck * n_h, outs, sh), F32),
                pltpu.VMEM((n_ck * n_h, outs, sh), BF16),
                pltpu.VMEM((n_ck * n_h, outs, sh), BF16),
                pltpu.VMEM((n_ck * n_h, outs, sh), BF16),
                pltpu.VMEM((n_ck * n_h, outs, sh), BF16),
                pltpu.VMEM((n_ck, outs, sh), F32),
                pltpu.VMEM((outs, local_pts), BF16),
                pltpu.VMEM((n_cc * n_dp, outs, cw), F32),
                pltpu.VMEM((n_cc * n_dp, outs, cw), F32),
                pltpu.VMEM((n_cc, outs, cw), F32),
                pltpu.VMEM((n_cc, n_dp, outs, cw), F32),
                pltpu.VMEM((2, 2, 2 * sh, width), BF16),
                pltpu.VMEM((outs, quarter), F32),
            ] + [dma((1,))] * 2 + [dma((n_ck * n_h,))] * 8 + [dma((n_h,))] * 8 + [dma((n_cc * n_dp,))] * 4,
            compiler_params=pltpu.CompilerParams(
                collective_id=0, has_side_effects=True, vmem_limit_bytes=40 * 1024 * 1024
            ),
        )(*args)
        return result.T

    return jax.shard_map(
        on_device,
        mesh=mesh,
        in_specs=(P("dp", None), P("centers", None), P("centers", None)),
        out_specs=P("centers", None),
        check_vma=False,
    )
```

```python
import functools
import math

import jax
import jax.numpy as jnp
from jax import lax
from jax.experimental import pallas as pl
from jax.experimental.pallas import tpu as pltpu
from jax.sharding import PartitionSpec as P

MESH = pl.DeviceIdType.MESH
F32, BF16 = jnp.float32, jnp.bfloat16
PIECE = 1024


def split3(v):
    hi = v.astype(BF16).astype(F32)
    mid = (v - hi).astype(BF16).astype(F32)
    return hi, mid, (v - hi) - mid


def row_form(xt, width):
    feats, count = xt.shape
    wide = xt.astype(F32)
    sq = jnp.sum(wide * wide, axis=0, keepdims=True) * (-2.0 * math.log2(math.e) / feats)
    hi, mid, lo = split3(sq)
    at = lax.broadcasted_iota(jnp.int32, (width - 3 * feats, count), 0)
    tail = jnp.where(at == 3, hi, jnp.where(at == 4, mid, jnp.where(at == 5, lo, 0.0)))
    tail = jnp.where(at < 3, 1.0, tail)
    return jnp.concatenate([xt, xt, xt, tail.astype(BF16)], axis=0).T


def col_form(ct, width):
    feats, count = ct.shape
    wide = ct.astype(F32)
    parts = [p.astype(BF16) for p in split3(wide * (4.0 * math.log2(math.e) / feats))]
    sq = jnp.sum(wide * wide, axis=0, keepdims=True) * (-2.0 * math.log2(math.e) / feats)
    hi, mid, lo = split3(sq)
    at = lax.broadcasted_iota(jnp.int32, (width - 3 * feats, count), 0)
    tail = jnp.where(at == 0, hi, jnp.where(at == 1, mid, jnp.where(at == 2, lo, 0.0)))
    tail = jnp.where((at >= 3) & (at < 6), 1.0, tail)
    return jnp.concatenate(parts + [tail.astype(BF16)], axis=0)


def xor(v, k):
    out, bit = v, 1
    while bit <= k:
        if k & bit:
            out = out + bit - 2 * bit * lax.rem(v // bit, 2)
        bit *= 2
    return out


class Mxu:
    def __init__(self, q, tiles, sums):
        self.q, self.tiles, self.sums, self.count = q, tiles, sums, 0

    def push(self, value, transpose=False):
        r = self.count % 2
        self.count += 1
        pltpu.matmul_push_rhs(value, staging_register=r, mxu_index=self.q, transpose=transpose)
        return r

    def stream(self, pairs, transpose):
        made = 0
        prev = []

        def use(item, r):
            pltpu.matmul_acc_lhs(self.sums[item[1][2]], item[1][3](), load_staged_rhs=r)

        def tile(item):
            value = jnp.exp2(pltpu.matmul_pop(self.tiles[item[0]])).astype(BF16)
            item[1][1](value)
            return self.push(value, transpose)

        r = self.push(pairs[0][0]())
        for i, (_, units) in enumerate(pairs):
            now = []
            for n in range(max(len(units), len(prev))):
                if n < len(units):
                    pltpu.matmul_acc_lhs(self.tiles[made % 3], units[n][0](), load_staged_rhs=r if n == 0 else None)
                    now.append((made % 3, units[n]))
                    made += 1
                    yield
                if n < len(prev):
                    prev[n] = prev[n] + (tile(prev[n]),)
                    yield
            for n, item in enumerate(prev):
                use(item, item[2])
                if n == 0 and i + 1 < len(pairs):
                    r = self.push(pairs[i + 1][0]())
                yield
            if not prev and i + 1 < len(pairs):
                r = self.push(pairs[i + 1][0]())
            prev = now
        prev = [item + (tile(item),) for item in prev]
        yield
        for item in prev:
            use(item, item[2])

    def chain(self, items):
        r = self.push(items[0][0]())
        for n, (_, rows, k) in enumerate(items):
            after = self.push(items[n + 1][0]()) if n + 1 < len(items) else None
            pltpu.matmul_acc_lhs(self.sums[k], rows(), load_staged_rhs=r)
            r = after
            yield


def together(streams):
    streams = list(streams)
    while streams:
        for stream in list(streams):
            if next(stream, streams) is streams:
                streams.remove(stream)


def inner(cfg, accs, pts_hbm, cen_hbm, coef_hbm, out, pts, packed, lsem, sibp, kmat, colt, gath, reg, own_half, snd1, rcv1, snd2, rcv2,
         own_sum, fwd, csend, crecv, cown, full, rowp, rowg, loc,
         os_, or_, b1s, b1r, b2s, b2r, gs, gr, hs, hr, ups, upr, dns, dnr, fus, fur, fds, fdr, cs, cr, ds_, dr):
    n_dp, n_c, feats, width, n_ck, n_cc = cfg
    mxu = [Mxu(q, accs[7 * q:7 * q + 3], accs[7 * q + 3:7 * q + 7]) for q in range(2)]
    n_h = n_c // 2
    d = lax.axis_index("dp")
    j = lax.axis_index("centers")
    par = lax.rem(j, 2)
    z = j // 2
    sib = j + 1 - 2 * par
    local_pts = pts.shape[1]
    local_cen = packed.shape[1]
    outs = packed.shape[0] - feats
    share = local_pts // n_c
    sh = share // n_ck
    span = n_c * sh
    quarter = local_cen // n_dp
    cw = quarter // n_cc
    piece = min(PIECE, local_cen)
    alpha_scale = 1.0 / math.sqrt(local_pts * n_dp)

    def copy(src, dst, ssem, rsem, dev):
        return pltpu.make_async_remote_copy(
            src_ref=src, dst_ref=dst, send_sem=ssem, recv_sem=rsem, device_id=dev, device_id_type=MESH
        )

    def peer(k):
        return (d, 2 * xor(z, k) + par)

    barrier = pltpu.get_barrier_semaphore()
    for k in range(1, n_h):
        pl.semaphore_signal(barrier, inc=1, device_id=peer(k), device_id_type=MESH)
    pl.semaphore_signal(barrier, inc=1, device_id=(d, sib), device_id_type=MESH)
    for k in range(1, n_dp):
        pl.semaphore_signal(barrier, inc=1, device_id=(xor(d, k), j), device_id_type=MESH)

    cen_in = pltpu.make_async_copy(cen_hbm, packed.at[:feats], lsem.at[0])
    coef_in = pltpu.make_async_copy(coef_hbm, packed.at[feats:], lsem.at[1])
    pts_in = pltpu.make_async_copy(pts_hbm, pts, lsem.at[2])
    cen_in.start()
    coef_in.start()
    pts_in.start()
    cen_in.wait()
    for c in range(local_cen // piece):
        at = pl.ds(c * piece, piece)
        colt[:width, at] = col_form(packed[:feats, at], width)
    colt[width:, :] = jnp.zeros_like(colt[width:, :])
    rowp[:, :, :, width:] = jnp.zeros_like(rowp[:, :, :, width:])
    reg[...] = jnp.zeros_like(reg)
    loc[...] = jnp.zeros_like(loc)
    coef_in.wait()
    pts_in.wait()

    mine = packed.at[:, pl.ds(pl.multiple_of(d * quarter, 128), quarter)]

    def up(r):
        dst = gath.at[2 * (z - r) + par]
        return copy(mine if r == 0 else dst, dst, ups.at[r], upr.at[r], (d, 2 * (z + 1) + par))

    def down(r):
        dst = gath.at[2 * (z + r) + par]
        return copy(mine if r == 0 else dst, dst, dns.at[r], dnr.at[r], (d, 2 * (z - 1) + par))

    def up_in(r):
        dst = gath.at[2 * (z - r) + par]
        return copy(dst, dst, ups.at[r - 1], upr.at[r - 1], (d, sib))

    def down_in(r):
        dst = gath.at[2 * (z + r) + par]
        return copy(dst, dst, dns.at[r - 1], dnr.at[r - 1], (d, sib))

    def below_sib(r):
        at = gath.at[2 * (z - r) + par]
        return copy(at, at, fus.at[r], fur.at[r], (d, sib))

    def above_sib(r):
        at = gath.at[2 * (z + r) + par]
        return copy(at, at, fds.at[r], fdr.at[r], (d, sib))

    def below_sib_in(r):
        at = gath.at[2 * (z - r) + 1 - par]
        return copy(at, at, fus.at[r], fur.at[r], (d, sib))

    def above_sib_in(r):
        at = gath.at[2 * (z + r) + 1 - par]
        return copy(at, at, fds.at[r], fdr.at[r], (d, sib))

    def hop(r):
        if r > 0:
            @pl.when(z >= r)
            def _():
                up_in(r).wait_recv()
                below_sib(r).start()

            @pl.when(z + r < n_h)
            def _():
                down_in(r).wait_recv()
                above_sib(r).start()

        if r < n_h - 1:
            @pl.when((z >= r) & (z < n_h - 1))
            def _():
                up(r).start()

            @pl.when((z + r < n_h) & (z > 0))
            def _():
                down(r).start()

    def hop_sib_in(r):
        @pl.when(z >= r)
        def _():
            below_sib_in(r).wait_recv()

        @pl.when(z + r < n_h)
        def _():
            above_sib_in(r).wait_recv()

    def hop_sent(r):
        if r > 0:
            @pl.when(z >= r)
            def _():
                below_sib(r).wait_send()

            @pl.when(z + r < n_h)
            def _():
                above_sib(r).wait_send()

        if r < n_h - 1:
            @pl.when((z >= r) & (z < n_h - 1))
            def _():
                up(r).wait_send()

            @pl.when((z + r < n_h) & (z > 0))
            def _():
                down(r).wait_send()

    own_to_sib = copy(packed, sibp, os_.at[0], or_.at[0], (d, sib))

    def to_sib(s):
        return copy(snd1.at[s], rcv1.at[s], b1s.at[s], b1r.at[s], (d, sib))

    def to_peer(c, k):
        i = c * n_h + k
        return copy(snd2.at[i], rcv2.at[i], b2s.at[i], b2r.at[i], peer(k))

    def slot(c, q):
        return fwd.at[:, pl.ds(pl.multiple_of(c * span + q * sh, sh), sh)]

    def spread(c, k):
        i = c * n_h + k
        return copy(slot(c, j), slot(c, j), gs.at[i], gr.at[i], peer(k))

    def spread_in(c, k):
        i = c * n_h + k
        at = slot(c, 2 * xor(z, k) + par)
        return copy(at, at, gs.at[i], gr.at[i], peer(k))

    def relay(c, k):
        i = c * n_h + k
        at = slot(c, 2 * xor(z, k) + par)
        return copy(at, at, hs.at[i], hr.at[i], (d, sib))

    def relay_in(c, k):
        i = c * n_h + k
        at = slot(c, 2 * xor(z, k) + 1 - par)
        return copy(at, at, hs.at[i], hr.at[i], (d, sib))

    steps = n_ck * n_h

    group = 2

    def owners(s):
        zt = xor(z, n_h - 1 - s % n_h)
        return 2 * zt + 1 - par, 2 * zt + par

    def point_rows(g):
        for i, s in enumerate(range(g * group, (g + 1) * group)):
            for h, q in enumerate(owners(s)):
                src = pl.ds(pl.multiple_of(q * share + (s // n_h) * sh, sh), sh)
                rowp[g % 2, i, h * sh:(h + 1) * sh, :width] = row_form(pts[:, src], width)

    def forward(g):
        if (g + 1) * group < steps:
            point_rows(g + 1)
        blocks = []
        for i, s in enumerate(range(g * group, (g + 1) * group)):
            ats = [pl.ds(pl.multiple_of((s // n_h) * span + q * sh, sh), sh) for q in owners(s)]
            for r in range(0, 2 * sh, 256):
                held = [(ats[h], h * sh - r) for h in range(2) if r <= h * sh < r + 256]
                blocks.append((s, i, r, held))
        plans = []
        for q in range(2):
            pairs = []
            for c in range(0, local_cen, 256):
                cols = pl.ds(c, 256)
                units = []
                for n, (s, i, r, held) in enumerate(blocks[q::2]):

                    def keep(tile, cols=cols, held=held):
                        for at, o in held:
                            kmat[at, cols] = tile[o:o + sh]

                    units.append((
                        lambda i=i, r=r: rowp[g % 2, i, r:r + 256, :], keep, n,
                        lambda cols=cols: packed[feats:, cols],
                    ))
                pairs.append((lambda cols=cols: colt[:, cols], units))
            plans.append(pairs)
        together(mxu[q].stream(plans[q], True) for q in range(2))
        for q in range(2):
            for n, (s, i, r, held) in enumerate(blocks[q::2]):
                total = pltpu.matmul_pop(mxu[q].sums[n])
                for at, o in held:
                    if r + o == 0:
                        snd1[s] = total[:, o:o + sh].astype(BF16)
                    else:
                        own_half[s] = total[:, o:o + sh]

    def combine(s):
        c, k = s // n_h, n_h - 1 - s % n_h
        to_sib(s).wait_recv()
        total = own_half[s] + rcv1[s].astype(F32)
        if k > 0:
            snd2[c * n_h + k] = total.astype(BF16)
            to_peer(c, k).start()
        else:
            own_sum[c] = total

    def finish(c):
        for k in range(1, n_h):
            to_peer(c, k).wait_recv()
        total = own_sum[c]
        for k in range(1, n_h):
            total = total + rcv2[c * n_h + k].astype(F32)
        slot(c, j)[...] = total.astype(BF16)
        for k in reversed(range(1, n_h)):
            spread(c, k).start()
        relay(c, 0).start()

    def relays(c):
        for k in range(1, n_h):
            spread_in(c, k).wait_recv()
            relay(c, k).start()

    def regular(*blocks):
        for i, block in enumerate(blocks):
            rowg[pl.ds(i * quarter, quarter), :width] = row_form(gath[block, :feats, :], width)
        plans = []
        for q in range(2):
            pairs = []
            for n, c in enumerate(range(q * 256, local_cen, 512)):
                cols = pl.ds(c, 256)
                for i, block in enumerate(blocks):
                    units = [(
                        lambda i=i, r=r: rowg[pl.ds(i * quarter + r, 256), :], lambda tile: None, n,
                        lambda block=block, r=r: gath[block, feats:, pl.ds(r, 256)],
                    ) for r in range(0, quarter, 256)]
                    pairs.append((lambda cols=cols: colt[:, cols], units))
            plans.append(pairs)
        together(mxu[q].stream(plans[q], False) for q in range(2))
        for q in range(2):
            for n, c in enumerate(range(q * 256, local_cen, 512)):
                reg[:, pl.ds(c, 256)] += pltpu.matmul_pop(mxu[q].sums[n])

    def back(c, cols):
        plans = []
        for q in range(2):
            plans.append([(
                lambda k=k, at=at: kmat[pl.ds(c * span + k * 256, 256), at],
                lambda k=k: fwd[:, pl.ds(c * span + k * 256, 256)], n,
            ) for n, at in enumerate(cols[q::2]) for k in range(span // 256)])
        together(mxu[q].chain(plans[q]) for q in range(2) if plans[q])
        return [pltpu.matmul_pop(mxu[i % 2].sums[i // 2]) * alpha_scale for i in range(len(cols))]

    hops = list(range(1, n_h))
    sib_hops = list(range(1, n_h))

    def ensure(r):
        while hops and hops[0] <= r:
            hop(hops.pop(0))

    def ensure_sib(r):
        ensure(r)
        while sib_hops and sib_hops[0] <= r:
            hop_sib_in(sib_hops.pop(0))

    own_cols = pl.ds(pl.multiple_of(d * quarter, 128), quarter)

    def local(src):
        rowg[:, :width] = row_form(src[:feats, :], width)
        n_rows = local_cen // 256
        plans = []
        for q in range(2):
            pairs = []
            for n, c in enumerate(range(0, quarter, 256)):
                cols = pl.ds(pl.multiple_of(d * quarter + c, 128), 256)
                for b in range(q, n_rows, 4):
                    units = [(
                        lambda r=r: rowg[pl.ds(r * 256, 256), :], lambda tile: None, n,
                        lambda r=r: src[feats:, pl.ds(r * 256, 256)],
                    ) for r in range(b, min(b + 4, n_rows), 2)]
                    pairs.append((lambda cols=cols: colt[:, cols], units))
            plans.append(pairs)
        together(mxu[q].stream(plans[q], False) for q in range(2))
        for n, c in enumerate(range(0, quarter, 256)):
            loc[:, c:c + 256] += pltpu.matmul_pop(mxu[0].sums[n]) + pltpu.matmul_pop(mxu[1].sums[n])

    last = n_ck - 1
    groups = steps // group
    point_rows(0)
    for g in range(groups):
        forward(g)
        if g == 0:
            rowg[:, width:] = jnp.zeros_like(rowg[:, width:])
            pl.semaphore_wait(barrier, n_h - 1 + 1 + n_dp - 1)
        for s in range(g * group, (g + 1) * group):
            to_sib(s).start()
        if g == 0:
            hop(0)
        if g > 0:
            for s in range((g - 1) * group, g * group):
                combine(s)
        if g == groups - 2:
            ensure(1)
            own_to_sib.start()
    near = 2 * xor(z, 1)
    ensure_sib(1)
    regular(near + par)
    for s in range(steps - group, steps):
        combine(s)
    if n_ck > 1:
        finish(0)
    regular(near + 1 - par)
    ensure(2)
    finish(last)
    rest = list(range(2, n_h))
    for k in rest[:-1]:
        ensure(k)
        regular(2 * xor(z, k) + par)
        ensure_sib(k)
        regular(2 * xor(z, k) + 1 - par)
    if n_ck > 1:
        relays(0)
        for k in rest[-1:]:
            ensure(k)
        for k in range(n_h):
            relay_in(0, k).wait_recv()
        cols = [pl.ds(b, 256) for b in range(0, local_cen, 256)]
        for at, value in zip(cols, back(0, cols)):
            reg[:, at] += value
    for k in rest[-1:]:
        ensure(k)
        relays(last)
        ensure_sib(k)
        regular(2 * xor(z, k) + par, 2 * xor(z, k) + 1 - par)
    if not rest:
        relays(last)
    for k in range(n_h):
        relay_in(last, k).wait_recv()

    def cross(cc, k):
        i = cc * n_dp + k
        return copy(csend.at[i], crecv.at[i], cs.at[i], cr.at[i], (xor(d, k), j))

    for cc in range(n_cc):
        for first in range(n_dp - 1, -1, -2):
            order = [first, first - 1]
            ats = [pl.ds(pl.multiple_of(xor(d, k) * quarter + cc * cw, 128), cw) for k in order]
            for k, at, value in zip(order, ats, back(last, ats)):
                total = value + reg[:, at]
                if k > 0:
                    csend[cc * n_dp + k] = total
                else:
                    cown[cc] = total
            for k in order:
                if k > 0:
                    cross(cc, k).start()

    local(packed)
    own_to_sib.wait_recv()
    local(sibp)

    def publish(cc, k):
        i = cc * n_dp + k
        at = full.at[cc, d]
        return copy(at, at, ds_.at[i], dr.at[i], (xor(d, k), j))

    def publish_in(cc, k):
        i = cc * n_dp + k
        at = full.at[cc, xor(d, k)]
        return copy(at, at, ds_.at[i], dr.at[i], (xor(d, k), j))

    for cc in range(n_cc):
        for k in range(1, n_dp):
            cross(cc, k).wait_recv()
        total = cown[cc] + loc[:, cc * cw:(cc + 1) * cw]
        for k in range(1, n_dp):
            total = total + crecv[cc * n_dp + k]
        full[cc, d] = total
        for k in reversed(range(1, n_dp)):
            publish(cc, k).start()

    for r in range(n_h):
        hop_sent(r)
    for s in range(steps):
        to_sib(s).wait_send()
    own_to_sib.wait_send()
    for c in range(n_ck):
        relay(c, 0).wait_send()
        for k in range(1, n_h):
            to_peer(c, k).wait_send()
            spread(c, k).wait_send()
            relay(c, k).wait_send()
    for cc in range(n_cc):
        for k in range(1, n_dp):
            cross(cc, k).wait_send()
            publish_in(cc, k).wait_recv()
        for q in range(n_dp):
            out[:, q * quarter + cc * cw:q * quarter + (cc + 1) * cw] = full[cc, q]
    for cc in range(n_cc):
        for k in range(1, n_dp):
            publish(cc, k).wait_send()


def body(cfg, *refs):
    def run(*accs):
        inner(cfg, accs, *refs)

    specs = []
    for q in range(2):
        specs += [pltpu.ACC(q)((256, 256), F32)] * 3 + [pltpu.ACC(q)((64, 256), F32)] * 4
    pl.run_scoped(run, *specs)


def solution(mesh):
    n_dp, n_c = mesh.shape["dp"], mesh.shape["centers"]

    def on_device(points, centers, coef):
        local_pts, feats = points.shape
        local_cen, outs = coef.shape
        width = -(-(3 * feats + 6) // 128) * 128
        n_h = n_c // 2
        share, quarter = local_pts // n_c, local_cen // n_dp
        n_ck = 2 if share % 256 == 0 else 1
        n_cc = quarter // 256
        sh, cw = share // n_ck, quarter // n_cc
        dma = pltpu.SemaphoreType.DMA
        args = [pltpu.with_memory_space_constraint(v.T, pltpu.HBM) for v in (points, centers, coef)]
        result = pl.pallas_call(
            functools.partial(body, (n_dp, n_c, feats, width, n_ck, n_cc)),
            out_shape=jax.ShapeDtypeStruct((outs, local_cen), F32),
            in_specs=[pl.BlockSpec(memory_space=pl.ANY)] * 3,
            out_specs=pl.BlockSpec(memory_space=pltpu.VMEM),
            scratch_shapes=[
                pltpu.VMEM((feats, local_pts), BF16),
                pltpu.VMEM((feats + outs, local_cen), BF16),
                dma((3,)),
                pltpu.VMEM((feats + outs, local_cen), BF16),
                pltpu.VMEM((local_pts, local_cen), BF16),
                pltpu.VMEM((256, local_cen), BF16),
                pltpu.VMEM((n_c, feats + outs, quarter), BF16),
                pltpu.VMEM((outs, local_cen), F32),
                pltpu.VMEM((n_ck * n_h, outs, sh), F32),
                pltpu.VMEM((n_ck * n_h, outs, sh), BF16),
                pltpu.VMEM((n_ck * n_h, outs, sh), BF16),
                pltpu.VMEM((n_ck * n_h, outs, sh), BF16),
                pltpu.VMEM((n_ck * n_h, outs, sh), BF16),
                pltpu.VMEM((n_ck, outs, sh), F32),
                pltpu.VMEM((outs, local_pts), BF16),
                pltpu.VMEM((n_cc * n_dp, outs, cw), F32),
                pltpu.VMEM((n_cc * n_dp, outs, cw), F32),
                pltpu.VMEM((n_cc, outs, cw), F32),
                pltpu.VMEM((n_cc, n_dp, outs, cw), F32),
                pltpu.VMEM((2, 2, 2 * sh, 256), BF16),
                pltpu.VMEM((local_cen, 256), BF16),
                pltpu.VMEM((outs, quarter), F32),
            ] + [dma((1,))] * 2 + [dma((n_ck * n_h,))] * 8 + [dma((n_h,))] * 8 + [dma((n_cc * n_dp,))] * 4,
            compiler_params=pltpu.CompilerParams(
                collective_id=0, has_side_effects=True, vmem_limit_bytes=40 * 1024 * 1024
            ),
        )(*args)
        return result.T

    return jax.shard_map(
        on_device,
        mesh=mesh,
        in_specs=(P("dp", None), P("centers", None), P("centers", None)),
        out_specs=P("centers", None),
        check_vma=False,
    )
```

```python
import functools
import math

import jax
import jax.numpy as jnp
from jax import lax
from jax.experimental import pallas as pl
from jax.experimental.pallas import tpu as pltpu
from jax.sharding import PartitionSpec as P

MESH = pl.DeviceIdType.MESH
F32, BF16 = jnp.float32, jnp.bfloat16
PIECE = 1024


def split3(v):
    hi = v.astype(BF16).astype(F32)
    mid = (v - hi).astype(BF16).astype(F32)
    return hi, mid, (v - hi) - mid


def row_form(xt, width):
    feats, count = xt.shape
    wide = xt.astype(F32)
    sq = jnp.sum(wide * wide, axis=0, keepdims=True) * (-2.0 * math.log2(math.e) / feats)
    hi, mid, lo = split3(sq)
    at = lax.broadcasted_iota(jnp.int32, (width - 3 * feats, count), 0)
    tail = jnp.where(at == 3, hi, jnp.where(at == 4, mid, jnp.where(at == 5, lo, 0.0)))
    tail = jnp.where(at < 3, 1.0, tail)
    return jnp.concatenate([xt, xt, xt, tail.astype(BF16)], axis=0).T


def col_form(ct, width):
    feats, count = ct.shape
    wide = ct.astype(F32)
    parts = [p.astype(BF16) for p in split3(wide * (4.0 * math.log2(math.e) / feats))]
    sq = jnp.sum(wide * wide, axis=0, keepdims=True) * (-2.0 * math.log2(math.e) / feats)
    hi, mid, lo = split3(sq)
    at = lax.broadcasted_iota(jnp.int32, (width - 3 * feats, count), 0)
    tail = jnp.where(at == 0, hi, jnp.where(at == 1, mid, jnp.where(at == 2, lo, 0.0)))
    tail = jnp.where((at >= 3) & (at < 6), 1.0, tail)
    return jnp.concatenate(parts + [tail.astype(BF16)], axis=0)


def xor(v, k):
    out, bit = v, 1
    while bit <= k:
        if k & bit:
            out = out + bit - 2 * bit * lax.rem(v // bit, 2)
        bit *= 2
    return out


class Mxu:
    def __init__(self, q, tiles, sums):
        self.q, self.tiles, self.sums, self.count = q, tiles, sums, 0

    def push(self, value, transpose=False):
        r = self.count % 2
        self.count += 1
        pltpu.matmul_push_rhs(value, staging_register=r, mxu_index=self.q, transpose=transpose)
        return r

    def stream(self, pairs, transpose):
        made = 0
        prev = []

        def use(item, r):
            pltpu.matmul_acc_lhs(self.sums[item[1][2]], item[1][3](), load_staged_rhs=r)

        def tile(item):
            value = jnp.exp2(pltpu.matmul_pop(self.tiles[item[0]])).astype(BF16)
            item[1][1](value)
            return self.push(value, transpose)

        r = self.push(pairs[0][0]())
        for i, (_, units) in enumerate(pairs):
            now = []
            for n in range(max(len(units), len(prev))):
                if n < len(units):
                    pltpu.matmul_acc_lhs(self.tiles[made % 3], units[n][0](), load_staged_rhs=r if n == 0 else None)
                    now.append((made % 3, units[n]))
                    made += 1
                    yield
                if n < len(prev):
                    prev[n] = prev[n] + (tile(prev[n]),)
                    yield
            for n, item in enumerate(prev):
                use(item, item[2])
                if n == 0 and i + 1 < len(pairs):
                    r = self.push(pairs[i + 1][0]())
                yield
            if not prev and i + 1 < len(pairs):
                r = self.push(pairs[i + 1][0]())
            prev = now
        prev = [item + (tile(item),) for item in prev]
        yield
        for item in prev:
            use(item, item[2])

    def chain(self, items):
        r = self.push(items[0][0]())
        for n, (_, rows, k) in enumerate(items):
            after = self.push(items[n + 1][0]()) if n + 1 < len(items) else None
            pltpu.matmul_acc_lhs(self.sums[k], rows(), load_staged_rhs=r)
            r = after
            yield


def together(streams):
    streams = list(streams)
    while streams:
        for stream in list(streams):
            if next(stream, streams) is streams:
                streams.remove(stream)


def inner(cfg, accs, pts_hbm, cen_hbm, coef_hbm, out, pts, packed, lsem, sibp, kmat, colt, gath, reg, own_half, snd1, rcv1, snd2, rcv2,
         own_sum, fwd, csend, crecv, cown, full, rowp, rowg, loc,
         os_, or_, b1s, b1r, b2s, b2r, gs, gr, hs, hr, ups, upr, dns, dnr, fus, fur, fds, fdr, cs, cr, ds_, dr):
    n_dp, n_c, feats, width, n_ck, n_cc = cfg
    mxu = [Mxu(q, accs[7 * q:7 * q + 3], accs[7 * q + 3:7 * q + 7]) for q in range(2)]
    n_h = n_c // 2
    d = lax.axis_index("dp")
    j = lax.axis_index("centers")
    par = lax.rem(j, 2)
    z = j // 2
    sib = j + 1 - 2 * par
    local_pts = pts.shape[1]
    local_cen = packed.shape[1]
    outs = packed.shape[0] - feats
    share = local_pts // n_c
    sh = share // n_ck
    span = n_c * sh
    quarter = local_cen // n_dp
    cw = quarter // n_cc
    piece = min(PIECE, local_cen)
    alpha_scale = 1.0 / math.sqrt(local_pts * n_dp)

    def copy(src, dst, ssem, rsem, dev):
        return pltpu.make_async_remote_copy(
            src_ref=src, dst_ref=dst, send_sem=ssem, recv_sem=rsem, device_id=dev, device_id_type=MESH
        )

    def peer(k):
        return (d, 2 * xor(z, k) + par)

    barrier = pltpu.get_barrier_semaphore()
    for k in range(1, n_h):
        pl.semaphore_signal(barrier, inc=1, device_id=peer(k), device_id_type=MESH)
    pl.semaphore_signal(barrier, inc=1, device_id=(d, sib), device_id_type=MESH)
    for k in range(1, n_dp):
        pl.semaphore_signal(barrier, inc=1, device_id=(xor(d, k), j), device_id_type=MESH)

    cen_in = pltpu.make_async_copy(cen_hbm, packed.at[:feats], lsem.at[0])
    coef_in = pltpu.make_async_copy(coef_hbm, packed.at[feats:], lsem.at[1])
    pts_in = pltpu.make_async_copy(pts_hbm, pts, lsem.at[2])
    cen_in.start()
    coef_in.start()
    pts_in.start()
    cen_in.wait()
    for c in range(local_cen // piece):
        at = pl.ds(c * piece, piece)
        colt[:width, at] = col_form(packed[:feats, at], width)
    colt[width:, :] = jnp.zeros_like(colt[width:, :])
    rowp[:, :, :, width:] = jnp.zeros_like(rowp[:, :, :, width:])
    reg[...] = jnp.zeros_like(reg)
    loc[...] = jnp.zeros_like(loc)
    coef_in.wait()
    pts_in.wait()

    mine = packed.at[:, pl.ds(pl.multiple_of(d * quarter, 128), quarter)]

    def up(r):
        dst = gath.at[2 * (z - r) + par]
        return copy(mine if r == 0 else dst, dst, ups.at[r], upr.at[r], (d, 2 * (z + 1) + par))

    def down(r):
        dst = gath.at[2 * (z + r) + par]
        return copy(mine if r == 0 else dst, dst, dns.at[r], dnr.at[r], (d, 2 * (z - 1) + par))

    def up_in(r):
        dst = gath.at[2 * (z - r) + par]
        return copy(dst, dst, ups.at[r - 1], upr.at[r - 1], (d, sib))

    def down_in(r):
        dst = gath.at[2 * (z + r) + par]
        return copy(dst, dst, dns.at[r - 1], dnr.at[r - 1], (d, sib))

    def below_sib(r):
        at = gath.at[2 * (z - r) + par]
        return copy(at, at, fus.at[r], fur.at[r], (d, sib))

    def above_sib(r):
        at = gath.at[2 * (z + r) + par]
        return copy(at, at, fds.at[r], fdr.at[r], (d, sib))

    def below_sib_in(r):
        at = gath.at[2 * (z - r) + 1 - par]
        return copy(at, at, fus.at[r], fur.at[r], (d, sib))

    def above_sib_in(r):
        at = gath.at[2 * (z + r) + 1 - par]
        return copy(at, at, fds.at[r], fdr.at[r], (d, sib))

    def hop(r):
        if r > 0:
            @pl.when(z >= r)
            def _():
                up_in(r).wait_recv()
                below_sib(r).start()

            @pl.when(z + r < n_h)
            def _():
                down_in(r).wait_recv()
                above_sib(r).start()

        if r < n_h - 1:
            @pl.when((z >= r) & (z < n_h - 1))
            def _():
                up(r).start()

            @pl.when((z + r < n_h) & (z > 0))
            def _():
                down(r).start()

    def hop_sib_in(r):
        @pl.when(z >= r)
        def _():
            below_sib_in(r).wait_recv()

        @pl.when(z + r < n_h)
        def _():
            above_sib_in(r).wait_recv()

    def hop_sent(r):
        if r > 0:
            @pl.when(z >= r)
            def _():
                below_sib(r).wait_send()

            @pl.when(z + r < n_h)
            def _():
                above_sib(r).wait_send()

        if r < n_h - 1:
            @pl.when((z >= r) & (z < n_h - 1))
            def _():
                up(r).wait_send()

            @pl.when((z + r < n_h) & (z > 0))
            def _():
                down(r).wait_send()

    own_to_sib = copy(packed, sibp, os_.at[0], or_.at[0], (d, sib))

    def to_sib(s):
        return copy(snd1.at[s], rcv1.at[s], b1s.at[s], b1r.at[s], (d, sib))

    def to_peer(c, k):
        i = c * n_h + k
        return copy(snd2.at[i], rcv2.at[i], b2s.at[i], b2r.at[i], peer(k))

    def slot(c, q):
        return fwd.at[:, pl.ds(pl.multiple_of(c * span + q * sh, sh), sh)]

    def spread(c, k):
        i = c * n_h + k
        return copy(slot(c, j), slot(c, j), gs.at[i], gr.at[i], peer(k))

    def spread_in(c, k):
        i = c * n_h + k
        at = slot(c, 2 * xor(z, k) + par)
        return copy(at, at, gs.at[i], gr.at[i], peer(k))

    def relay(c, k):
        i = c * n_h + k
        at = slot(c, 2 * xor(z, k) + par)
        return copy(at, at, hs.at[i], hr.at[i], (d, sib))

    def relay_in(c, k):
        i = c * n_h + k
        at = slot(c, 2 * xor(z, k) + 1 - par)
        return copy(at, at, hs.at[i], hr.at[i], (d, sib))

    steps = n_ck * n_h

    group = 2

    def owners(s):
        zt = xor(z, n_h - 1 - s % n_h)
        return 2 * zt + 1 - par, 2 * zt + par

    def point_rows(g):
        for i, s in enumerate(range(g * group, (g + 1) * group)):
            for h, q in enumerate(owners(s)):
                src = pl.ds(pl.multiple_of(q * share + (s // n_h) * sh, sh), sh)
                rowp[g % 2, i, h * sh:(h + 1) * sh, :width] = row_form(pts[:, src], width)

    def forward(g):
        if (g + 1) * group < steps:
            point_rows(g + 1)
        blocks = []
        for i, s in enumerate(range(g * group, (g + 1) * group)):
            ats = [pl.ds(pl.multiple_of((s // n_h) * span + q * sh, sh), sh) for q in owners(s)]
            for r in range(0, 2 * sh, 256):
                held = [(ats[h], h * sh - r) for h in range(2) if r <= h * sh < r + 256]
                blocks.append((s, i, r, held))
        plans = []
        for q in range(2):
            pairs = []
            for c in range(0, local_cen, 256):
                cols = pl.ds(c, 256)
                units = []
                for n, (s, i, r, held) in enumerate(blocks[q::2]):

                    def keep(tile, cols=cols, held=held):
                        for at, o in held:
                            kmat[at, cols] = tile[o:o + sh]

                    units.append((
                        lambda i=i, r=r: rowp[g % 2, i, r:r + 256, :], keep, n,
                        lambda cols=cols: packed[feats:, cols],
                    ))
                pairs.append((lambda cols=cols: colt[:, cols], units))
            plans.append(pairs)
        together(mxu[q].stream(plans[q], True) for q in range(2))
        for q in range(2):
            for n, (s, i, r, held) in enumerate(blocks[q::2]):
                total = pltpu.matmul_pop(mxu[q].sums[n])
                for at, o in held:
                    if r + o == 0:
                        snd1[s] = total[:, o:o + sh].astype(BF16)
                    else:
                        own_half[s] = total[:, o:o + sh]

    def combine(s):
        c, k = s // n_h, n_h - 1 - s % n_h
        to_sib(s).wait_recv()
        total = own_half[s] + rcv1[s].astype(F32)
        if k > 0:
            snd2[c * n_h + k] = total.astype(BF16)
            to_peer(c, k).start()
        else:
            own_sum[c] = total

    def finish(c):
        for k in range(1, n_h):
            to_peer(c, k).wait_recv()
        total = own_sum[c]
        for k in range(1, n_h):
            total = total + rcv2[c * n_h + k].astype(F32)
        slot(c, j)[...] = total.astype(BF16)
        for k in reversed(range(1, n_h)):
            spread(c, k).start()
        relay(c, 0).start()

    def relays(c):
        for k in range(1, n_h):
            spread_in(c, k).wait_recv()
            relay(c, k).start()

    def regular(*blocks):
        for i, block in enumerate(blocks):
            rowg[pl.ds(i * quarter, quarter), :width] = row_form(gath[block, :feats, :], width)
        plans = []
        for q in range(2):
            pairs = []
            for n, c in enumerate(range(q * 256, local_cen, 512)):
                cols = pl.ds(c, 256)
                for i, block in enumerate(blocks):
                    units = [(
                        lambda i=i, r=r: rowg[pl.ds(i * quarter + r, 256), :], lambda tile: None, n,
                        lambda block=block, r=r: gath[block, feats:, pl.ds(r, 256)],
                    ) for r in range(0, quarter, 256)]
                    pairs.append((lambda cols=cols: colt[:, cols], units))
            plans.append(pairs)
        together(mxu[q].stream(plans[q], False) for q in range(2))
        for q in range(2):
            for n, c in enumerate(range(q * 256, local_cen, 512)):
                reg[:, pl.ds(c, 256)] += pltpu.matmul_pop(mxu[q].sums[n])

    def back(c, cols):
        plans = []
        for q in range(2):
            plans.append([(
                lambda k=k, at=at: kmat[pl.ds(c * span + k * 256, 256), at],
                lambda k=k: fwd[:, pl.ds(c * span + k * 256, 256)], n,
            ) for n, at in enumerate(cols[q::2]) for k in range(span // 256)])
        together(mxu[q].chain(plans[q]) for q in range(2) if plans[q])
        return [pltpu.matmul_pop(mxu[i % 2].sums[i // 2]) * alpha_scale for i in range(len(cols))]

    hops = list(range(1, n_h))
    sib_hops = list(range(1, n_h))

    def ensure(r):
        while hops and hops[0] <= r:
            hop(hops.pop(0))

    def ensure_sib(r):
        ensure(r)
        while sib_hops and sib_hops[0] <= r:
            hop_sib_in(sib_hops.pop(0))

    own_cols = pl.ds(pl.multiple_of(d * quarter, 128), quarter)

    def local(src):
        rowg[:, :width] = row_form(src[:feats, :], width)
        n_rows = local_cen // 256
        plans = []
        for q in range(2):
            pairs = []
            for n, c in enumerate(range(0, quarter, 256)):
                cols = pl.ds(pl.multiple_of(d * quarter + c, 128), 256)
                for b in range(q, n_rows, 4):
                    units = [(
                        lambda r=r: rowg[pl.ds(r * 256, 256), :], lambda tile: None, n,
                        lambda r=r: src[feats:, pl.ds(r * 256, 256)],
                    ) for r in range(b, min(b + 4, n_rows), 2)]
                    pairs.append((lambda cols=cols: colt[:, cols], units))
            plans.append(pairs)
        together(mxu[q].stream(plans[q], False) for q in range(2))
        for n, c in enumerate(range(0, quarter, 256)):
            loc[:, c:c + 256] += pltpu.matmul_pop(mxu[0].sums[n]) + pltpu.matmul_pop(mxu[1].sums[n])

    last = n_ck - 1
    groups = steps // group
    pl.semaphore_wait(barrier, n_h - 1 + 1 + n_dp - 1)
    hop(0)
    point_rows(0)
    for g in range(groups):
        forward(g)
        if g == 0:
            rowg[:, width:] = jnp.zeros_like(rowg[:, width:])
        for s in range(g * group, (g + 1) * group):
            to_sib(s).start()
        if g > 0:
            for s in range((g - 1) * group, g * group):
                combine(s)
        if g == max(groups - 3, 0):
            ensure(1)
            own_to_sib.start()
    near = 2 * xor(z, 1)
    ensure_sib(1)
    regular(near + par)
    for s in range(steps - group, steps):
        combine(s)
    if n_ck > 1:
        finish(0)
    ensure(2)
    regular(near + 1 - par)
    finish(last)
    rest = list(range(2, n_h))
    for k in rest[:-1]:
        ensure(k)
        regular(2 * xor(z, k) + par)
        ensure_sib(k)
        regular(2 * xor(z, k) + 1 - par)
    if n_ck > 1:
        relays(0)
        for k in rest[-1:]:
            ensure(k)
        for k in range(n_h):
            relay_in(0, k).wait_recv()
        cols = [pl.ds(b, 256) for b in range(0, local_cen, 256)]
        for at, value in zip(cols, back(0, cols)):
            reg[:, at] += value
    for k in rest[-1:]:
        ensure(k)
        relays(last)
        ensure_sib(k)
        regular(2 * xor(z, k) + par, 2 * xor(z, k) + 1 - par)
    if not rest:
        relays(last)
    for k in range(n_h):
        relay_in(last, k).wait_recv()

    def cross(cc, k):
        i = cc * n_dp + k
        return copy(csend.at[i], crecv.at[i], cs.at[i], cr.at[i], (xor(d, k), j))

    for cc in range(n_cc):
        for first in range(n_dp - 1, -1, -2):
            order = [first, first - 1]
            ats = [pl.ds(pl.multiple_of(xor(d, k) * quarter + cc * cw, 128), cw) for k in order]
            for k, at, value in zip(order, ats, back(last, ats)):
                total = value + reg[:, at]
                if k > 0:
                    csend[cc * n_dp + k] = total
                else:
                    cown[cc] = total
            for k in order:
                if k > 0:
                    cross(cc, k).start()

    local(packed)
    own_to_sib.wait_recv()
    local(sibp)

    def publish(cc, k):
        i = cc * n_dp + k
        at = full.at[cc, d]
        return copy(at, at, ds_.at[i], dr.at[i], (xor(d, k), j))

    def publish_in(cc, k):
        i = cc * n_dp + k
        at = full.at[cc, xor(d, k)]
        return copy(at, at, ds_.at[i], dr.at[i], (xor(d, k), j))

    for cc in range(n_cc):
        for k in range(1, n_dp):
            cross(cc, k).wait_recv()
        total = cown[cc] + loc[:, cc * cw:(cc + 1) * cw]
        for k in range(1, n_dp):
            total = total + crecv[cc * n_dp + k]
        full[cc, d] = total
        for k in reversed(range(1, n_dp)):
            publish(cc, k).start()

    for r in range(n_h):
        hop_sent(r)
    for s in range(steps):
        to_sib(s).wait_send()
    own_to_sib.wait_send()
    for c in range(n_ck):
        relay(c, 0).wait_send()
        for k in range(1, n_h):
            to_peer(c, k).wait_send()
            spread(c, k).wait_send()
            relay(c, k).wait_send()
    for cc in range(n_cc):
        for k in range(1, n_dp):
            cross(cc, k).wait_send()
            publish_in(cc, k).wait_recv()
        for q in range(n_dp):
            out[:, q * quarter + cc * cw:q * quarter + (cc + 1) * cw] = full[cc, q]
    for cc in range(n_cc):
        for k in range(1, n_dp):
            publish(cc, k).wait_send()


def body(cfg, *refs):
    def run(*accs):
        inner(cfg, accs, *refs)

    specs = []
    for q in range(2):
        specs += [pltpu.ACC(q)((256, 256), F32)] * 3 + [pltpu.ACC(q)((64, 256), F32)] * 4
    pl.run_scoped(run, *specs)


def solution(mesh):
    n_dp, n_c = mesh.shape["dp"], mesh.shape["centers"]

    def on_device(points, centers, coef):
        local_pts, feats = points.shape
        local_cen, outs = coef.shape
        width = -(-(3 * feats + 6) // 128) * 128
        n_h = n_c // 2
        share, quarter = local_pts // n_c, local_cen // n_dp
        n_ck = 2 if share % 256 == 0 else 1
        n_cc = quarter // 256
        sh, cw = share // n_ck, quarter // n_cc
        dma = pltpu.SemaphoreType.DMA
        args = [pltpu.with_memory_space_constraint(v.T, pltpu.HBM) for v in (points, centers, coef)]
        result = pl.pallas_call(
            functools.partial(body, (n_dp, n_c, feats, width, n_ck, n_cc)),
            out_shape=jax.ShapeDtypeStruct((outs, local_cen), F32),
            in_specs=[pl.BlockSpec(memory_space=pl.ANY)] * 3,
            out_specs=pl.BlockSpec(memory_space=pltpu.VMEM),
            scratch_shapes=[
                pltpu.VMEM((feats, local_pts), BF16),
                pltpu.VMEM((feats + outs, local_cen), BF16),
                dma((3,)),
                pltpu.VMEM((feats + outs, local_cen), BF16),
                pltpu.VMEM((local_pts, local_cen), BF16),
                pltpu.VMEM((256, local_cen), BF16),
                pltpu.VMEM((n_c, feats + outs, quarter), BF16),
                pltpu.VMEM((outs, local_cen), F32),
                pltpu.VMEM((n_ck * n_h, outs, sh), F32),
                pltpu.VMEM((n_ck * n_h, outs, sh), BF16),
                pltpu.VMEM((n_ck * n_h, outs, sh), BF16),
                pltpu.VMEM((n_ck * n_h, outs, sh), BF16),
                pltpu.VMEM((n_ck * n_h, outs, sh), BF16),
                pltpu.VMEM((n_ck, outs, sh), F32),
                pltpu.VMEM((outs, local_pts), BF16),
                pltpu.VMEM((n_cc * n_dp, outs, cw), F32),
                pltpu.VMEM((n_cc * n_dp, outs, cw), F32),
                pltpu.VMEM((n_cc, outs, cw), F32),
                pltpu.VMEM((n_cc, n_dp, outs, cw), F32),
                pltpu.VMEM((2, 2, 2 * sh, 256), BF16),
                pltpu.VMEM((local_cen, 256), BF16),
                pltpu.VMEM((outs, quarter), F32),
            ] + [dma((1,))] * 2 + [dma((n_ck * n_h,))] * 8 + [dma((n_h,))] * 8 + [dma((n_cc * n_dp,))] * 4,
            compiler_params=pltpu.CompilerParams(
                collective_id=0, has_side_effects=True, vmem_limit_bytes=40 * 1024 * 1024
            ),
        )(*args)
        return result.T

    return jax.shard_map(
        on_device,
        mesh=mesh,
        in_specs=(P("dp", None), P("centers", None), P("centers", None)),
        out_specs=P("centers", None),
        check_vma=False,
    )
```
